512 devices in a mesh: freq: 8 (over y, z_hi), space: 64 (over z_lo, x, core).
Axes of the slice: x: 4, y: 4, z: 16 (z_hi: 2, z_lo: 8; z = z_hi * 8 + z_lo), core: 2. Of those that a mesh axis runs over, the one named last changes fastest.
Arguments:
- probes: float32 [2, 128, 128, 128], P(None, 'space'), may hold values from -6 to 6
- background: float32 [8, 2, 128, 128, 128], P('freq', None, 'space'), may hold values from -6 to 6
- medium: float32 [128, 128, 128], P('space'), may hold values from 0.5 to 2
- shifts: float32 [8, 2], P('freq'), may hold values from -1.25 to 1, as said below
- receivers: int32 [128, 128, 128], P('space'), may hold values 0 or 1
Outputs:
- hessian: float32 [2, 128, 128, 128], P(None, 'space', 'freq')
The draws below stay inside these ranges and needn't reach their ends.
Inputs may be any that keep to these rules, and one draw needn't show every extreme that they name: `shifts`: column 0 lies in [-1.25, -0.5], column 1 in [0.2, 1.0].
All inputs are finite; a program needn't handle non-finite values. No bound on the sum of `receivers` on one device may be relied on, other than what follows from the above.
Results may differ from the reference program's by a relative error of at most 0.00002.
Values sent between devices are 32-bit elements; how exact they have to be, the bound alone decides.
No kernel may reach another device: no remote copies, remote signals or barrier semaphores. Data moves between devices by JAX's collectives and lax.ppermute only.
A program may use at most 64 MiB of HBM per device.

```python
import math
import jax
import jax.numpy as jnp

NY = 128
NZ = 128
PROBES = 2
STEPS = 4
FREQS = 8
NX = 128


def draw_probes(key, part):
    shape = (PROBES, NX, NY, NZ)
    inner = jax.random.fold_in(key, 11)
    return jnp.clip(jax.random.normal(inner, shape, jnp.float32), -6.0, 6.0)


def draw_background(key, part):
    shape = (FREQS, 2, NX, NY, NZ)
    inner = jax.random.fold_in(key, 23)
    return jnp.clip(jax.random.normal(inner, shape, jnp.float32), -6.0, 6.0)


def draw_shifts(key, part):
    inner = jax.random.fold_in(key, 37)
    real_part = jax.random.uniform(jax.random.fold_in(inner, 1), (FREQS, 1), jnp.float32, -1.25, -0.5)
    imag_part = jax.random.uniform(jax.random.fold_in(inner, 2), (FREQS, 1), jnp.float32, 0.2, 1.0)
    return jnp.concatenate([real_part, imag_part], axis=1)


def plant(values, stream_key, least, largest):
    longest = values.shape.index(max(values.shape))
    spots = []
    for shift in (0, 1):
        where = [jax.random.randint(jax.random.fold_in(stream_key, axis), (), 0, length) for axis, length in enumerate(values.shape)]
        where[longest] = (where[longest] + shift) % values.shape[longest]
        spots.append(tuple(where))
    return values.at[spots[0]].set(least).at[spots[1]].set(largest)


def levels(key, shape, split, smallest, high):
    gain = 1.0
    for position, blocks in split:
        steps = jax.random.uniform(jax.random.fold_in(jax.random.fold_in(key, 6), position), (blocks,), jnp.float32, smallest / len(split), high / len(split))
        gain = gain * jnp.repeat(jnp.exp(steps), shape[position] // blocks).reshape((-1,) + (1,) * (len(shape) - 1 - position))
    return gain


def setup_inputs(seed: int = 0) -> dict:
    key_of = jax.random.split(jax.random.key(seed), 6)
    probes = draw_probes(jax.random.fold_in(key_of[5], 71), 0)
    background = draw_background(jax.random.fold_in(key_of[5], 71), 0)
    medium = jnp.clip(jnp.exp(math.log(2.0) - 1.3862944 * jax.random.uniform(key_of[2], (NX, NY, NZ), jnp.float32) ** levels(key_of[2], (NX, NY, NZ), ((0, 64),), -0.2, 0.2)), 0.5, 2.0)
    shifts = draw_shifts(jax.random.fold_in(key_of[5], 71), 0)
    receivers = plant((jax.random.randint(key_of[4], (NX, NY, NZ), 0, 4) < 3).astype(jnp.int32), jax.random.fold_in(key_of[4], 1), 0, 1)
    return dict(probes=probes, background=background, medium=medium, shifts=shifts, receivers=receivers)


OMEGA_RELAX = 0.8


def neighbours(extended):
    center = extended[:, :, 1:-1]
    beside_all = extended[:, :, 2:] + extended[:, :, :-2]
    pad_y_low = ((0, 0), (0, 0), (0, 0), (0, 1), (0, 0))
    pad_y_high = ((0, 0), (0, 0), (0, 0), (1, 0), (0, 0))
    pad_z_low = ((0, 0), (0, 0), (0, 0), (0, 0), (0, 1))
    pad_z_high = ((0, 0), (0, 0), (0, 0), (0, 0), (1, 0))
    beside_all = beside_all + jnp.pad(center[:, :, :, 1:], pad_y_low) + jnp.pad(center[:, :, :, :-1], pad_y_high)
    beside_all = beside_all + jnp.pad(center[:, :, :, :, 1:], pad_z_low) + jnp.pad(center[:, :, :, :, :-1], pad_z_high)
    return center, beside_all


def sweep_once(extended, factors, source):
    diag_re, diag_im, inv_re, inv_im = factors
    center, beside_all = neighbours(extended)
    resid_re = source[0] - (diag_re * center[0] - diag_im * center[1]) + beside_all[0]
    resid_im = source[1] - (diag_re * center[1] + diag_im * center[0]) + beside_all[1]
    return center + jnp.stack([inv_re * resid_re - inv_im * resid_im, inv_re * resid_im + inv_im * resid_re])


def coefficients(medium, shift_re, shift_im):
    diag_re = 6.0 + shift_re * medium
    diag_im = shift_im * medium
    denom = diag_re * diag_re + diag_im * diag_im
    return (diag_re, diag_im, OMEGA_RELAX * diag_re / denom, -OMEGA_RELAX * diag_im / denom)


def conjugate(factors):
    return (factors[0], -factors[1], factors[2], -factors[3])


def relax_all(source, factors):
    iterate = jnp.zeros(source.shape, jnp.float32)
    for repeat in range(STEPS):
        extended = jnp.pad(iterate, ((0, 0), (0, 0), (1, 1), (0, 0), (0, 0)))
        iterate = sweep_once(extended, factors, source)
    return iterate


def reference(probes, background, medium, shifts, receivers):
    listen = receivers.astype(jnp.float32)
    total = jnp.zeros(probes.shape, jnp.float32)
    for freq_index in range(FREQS):
        shift_re = shifts[freq_index, 0]
        shift_im = shifts[freq_index, 1]
        back_re = background[freq_index, 0]
        back_im = background[freq_index, 1]
        scaled_re = shift_re * back_re - shift_im * back_im
        scaled_im = shift_re * back_im + shift_im * back_re
        source = jnp.stack([scaled_re * probes, scaled_im * probes])
        factors = coefficients(medium, shift_re, shift_im)
        forward = relax_all(source, factors)
        adjoint_field = relax_all(listen * forward, conjugate(factors))
        total = total + scaled_re * adjoint_field[0] + scaled_im * adjoint_field[1]
    return total
```

```python
import functools

import jax
import jax.numpy as jnp
from jax import lax
from jax.experimental import pallas as pl
from jax.experimental.pallas import tpu as pltpu
from jax.sharding import PartitionSpec as P


OMEGA = 0.8
KEEP = 1.0 - OMEGA
TOP = 8
ROWS = 32


def multiply(x, y):
    return (x[0] * y[0] - x[1] * y[1], x[0] * y[1] + x[1] * y[0])


def multiply_conj(x, y):
    return (x[0] * y[0] + x[1] * y[1], x[0] * y[1] - x[1] * y[0])


def inverse(medium, shift_re, shift_im):
    diag_re = 6.0 + shift_re * medium
    diag_im = shift_im * medium
    scale = OMEGA / (diag_re * diag_re + diag_im * diag_im)
    return (diag_re * scale, -diag_im * scale)


def chunks(height):
    return [(r, min(ROWS, height - r)) for r in range(0, height, ROWS)]


def clear_edges(pad):
    height = pad.shape[-2] - 2 * TOP
    zero = jnp.zeros((TOP, pad.shape[-1]), jnp.float32)
    for part in range(pad.shape[0]):
        pad[part, 0:TOP] = zero
        pad[part, TOP + height :] = zero


def in_plane(pad, part, r, n):
    here = pad[part, TOP + r : TOP + r + n]
    width = here.shape[-1]
    lane = lax.broadcasted_iota(jnp.int32, here.shape, 1)
    left = jnp.where(lane == 0, 0.0, pltpu.roll(here, 1, 1))
    right = jnp.where(lane == width - 1, 0.0, pltpu.roll(here, width - 1, 1))
    above = pad[part, TOP + r - 1 : TOP + r - 1 + n]
    below = pad[part, TOP + r + 1 : TOP + r + 1 + n]
    return here, (left + right) + (above + below)


def complex_in_plane(pad, layer, r, n):
    re, sum_re = in_plane(pad, 2 * layer, r, n)
    im, sum_im = in_plane(pad, 2 * layer + 1, r, n)
    return (re, im), (sum_re, sum_im)


def store(ref, at, r, n, value):
    ref[at, r : r + n] = value[0]
    ref[at + 1, r : r + n] = value[1]


def load(ref, at, r, n):
    return (ref[at, r : r + n], ref[at + 1, r : r + n])


def add(x, y):
    return (x[0] + y[0], x[1] + y[1])


def scale(a, x):
    return (a * x[0], a * x[1])


def side():
    return lax.rem(lax.axis_index("space"), 2)


def has_partner():
    at = lax.axis_index("space")
    last = lax.axis_size("space") - 1
    return jnp.where((at == 0) | (at == last), 0.0, 1.0).astype(jnp.float32)


def start_kernel(
    shifts_hbm, back_hbm, probes_hbm, medium_hbm, receivers_hbm,
    out_a0, out_a1, out_b, inv, waves, row,
    shifts, back, probes, medium, receivers, pad, sems,
):
    copies = [
        pltpu.make_async_copy(src, dst, sems.at[k])
        for k, (src, dst) in enumerate(
            (
                (shifts_hbm, shifts),
                (medium_hbm, medium),
                (back_hbm, back),
                (probes_hbm, probes),
                (receivers_hbm, receivers),
            )
        )
    ]
    for copy in copies:
        copy.start()
    near = side()
    own = (near, 1 - near)
    height = medium.shape[1]
    outs = ((out_a0, 0), (out_a1, 0)), ((out_b, 0), (out_b, 5))
    clear_edges(pad)
    copies[0].wait()
    shift_re, shift_im = shifts[0, 0], shifts[0, 1]
    row[0] = jnp.full(row.shape[1:], shift_re, jnp.float32)
    row[1] = jnp.full(row.shape[1:], shift_im, jnp.float32)
    copies[1].wait()
    for layer in range(2):
        for r, n in chunks(height):
            med = medium[own[layer], r : r + n]
            store(inv, 2 * layer, r, n, inverse(med, shift_re, shift_im))
            outs[layer][0][0][outs[layer][0][1] + 4, r : r + n] = med
    copies[2].wait()
    for layer in range(2):
        for r, n in chunks(height):
            rows = slice(r, r + n)
            bg = (back[0, 0, own[layer], rows], back[0, 1, own[layer], rows])
            store(waves, 2 * layer, r, n, multiply((shift_re, shift_im), bg))
    copies[3].wait()
    for p in range(2):
        for layer in range(2):
            ref, at = outs[layer][p]
            for r, n in chunks(height):
                probe = probes[p, own[layer], r : r + n]
                first = scale(probe, multiply(load(inv, 2 * layer, r, n), load(waves, 2 * layer, r, n)))
                store(ref, at, r, n, first)
                store(pad, 2 * layer, TOP + r, n, first)
        for layer in range(2):
            ref, at = outs[layer][p]
            for r, n in chunks(height):
                here, around = complex_in_plane(pad, layer, r, n)
                around = add(around, load(pad, 2 * (1 - layer), TOP + r, n))
                part = add(scale(1.0 + KEEP, here), multiply(load(inv, 2 * layer, r, n), around))
                store(ref, at + 2, r, n, part)
    copies[4].wait()
    for layer in range(2):
        ref, at = outs[layer][1]
        for r, n in chunks(height):
            ref[at + 4, r : r + n] = receivers[own[layer], r : r + n].astype(jnp.float32)


def halo_inverse(med, layer, row, mask):
    re, im = inverse(med, row[0, 0:1], row[1, 0:1])
    return (mask * re, mask * im) if layer == 0 else (re, im)


def forward_kernel(p, row, own_a, own_b, got_a, got_b, med_a, inv, *rest):
    if p == 0:
        out_a, out_b, pad, spare = rest
        b_at, out_at = 0, 0
    else:
        first_b, out_a, out_b, pad, spare = rest
        b_at, out_at = 5, 4
        out_b[0:4] = first_b[...]
    mask = has_partner()
    height = inv.shape[1]
    own = ((own_a, 0), (own_b, b_at))
    got = ((got_a, 0), (got_b, b_at))
    med = ((med_a, 4), (got_b, 4))
    out = ((out_a, 0), (out_b, out_at))
    clear_edges(pad)
    clear_edges(spare)
    for layer in range(2):
        (mine, at), (theirs, from_) = own[layer], got[layer]
        for r, n in chunks(height):
            second = add(
                load(mine, at + 2, r, n),
                multiply(load(inv, 2 * layer, r, n), load(theirs, from_, r, n)),
            )
            store(pad, 2 * layer, TOP + r, n, second)
    for layer in range(2):
        (mine, at), (theirs, from_) = own[layer], got[layer]
        for r, n in chunks(height):
            first = load(mine, at, r, n)
            there = halo_inverse(med[layer][0][med[layer][1], r : r + n], layer, row, mask)
            halo = add(load(theirs, from_ + 2, r, n), multiply(there, first))
            here, around = complex_in_plane(pad, layer, r, n)
            around = add(add(around, halo), load(pad, 2 * (1 - layer), TOP + r, n))
            third = add(
                add(scale(KEEP, here), first), multiply(load(inv, 2 * layer, r, n), around)
            )
            store(spare, 2 * layer, TOP + r, n, third)
            store(out[layer][0], out[layer][1], r, n, third)
    for layer in range(2):
        mine, at = own[layer]
        for r, n in chunks(height):
            here, around = complex_in_plane(spare, layer, r, n)
            around = add(around, load(spare, 2 * (1 - layer), TOP + r, n))
            part = add(
                add(scale(KEEP, here), load(mine, at, r, n)),
                multiply(load(inv, 2 * layer, r, n), around),
            )
            store(out[layer][0], out[layer][1] + 2, r, n, part)


def turn_kernel(
    p, row, own_a, own_b, got_a, got_b, med_a, got_b1, rec_a, own_a1, own_b1, inv, *rest
):
    if p == 0:
        out_a, out_b, right, pad, spare = rest
        b_at, out_at = 0, 0
    else:
        first_b, out_a, out_b, right, pad, spare = rest
        b_at, out_at = 4, 4
        out_b[0:4] = first_b[...]
    mask = has_partner()
    height = inv.shape[1]
    own = ((own_a, 0), (own_b, 0 if p == 0 else b_at))
    got = ((got_a, 0), (got_b, b_at))
    med = ((med_a, 4), (got_b1, 4))
    rec_own = ((own_a1, 4), (own_b1, 9))
    rec_got = ((rec_a, 4), (got_b1, 9))
    out = ((out_a, 0), (out_b, out_at))
    clear_edges(pad)
    clear_edges(spare)
    for layer in range(2):
        (mine, at), (theirs, from_) = own[layer], got[layer]
        for r, n in chunks(height):
            there = load(inv, 2 * layer, r, n)
            fourth = add(load(mine, at + 2, r, n), multiply(there, load(theirs, from_, r, n)))
            heard = scale(rec_own[layer][0][rec_own[layer][1], r : r + n], fourth)
            first = multiply_conj(there, heard)
            store(pad, 2 * layer, TOP + r, n, first)
            store(right, 2 * layer, r, n, first)
    for layer in range(2):
        (mine, at), (theirs, from_) = own[layer], got[layer]
        for r, n in chunks(height):
            there = halo_inverse(med[layer][0][med[layer][1], r : r + n], layer, row, mask)
            fourth = add(load(theirs, from_ + 2, r, n), multiply(there, load(mine, at, r, n)))
            halo = multiply_conj(
                there, scale(rec_got[layer][0][rec_got[layer][1], r : r + n], fourth)
            )
            here, around = complex_in_plane(pad, layer, r, n)
            around = add(add(around, halo), load(pad, 2 * (1 - layer), TOP + r, n))
            second = add(
                scale(1.0 + KEEP, here), multiply_conj(load(inv, 2 * layer, r, n), around)
            )
            store(spare, 2 * layer, TOP + r, n, second)
            store(out[layer][0], out[layer][1], r, n, second)
    for layer in range(2):
        for r, n in chunks(height):
            here, around = complex_in_plane(spare, layer, r, n)
            around = add(around, load(spare, 2 * (1 - layer), TOP + r, n))
            part = add(
                add(scale(KEEP, here), load(right, 2 * layer, r, n)),
                multiply_conj(load(inv, 2 * layer, r, n), around),
            )
            store(out[layer][0], out[layer][1] + 2, r, n, part)


def end_kernel(p, row, own_a, own_b, got_a, got_b, med_a, got_b1, inv, right, waves, *rest):
    if p == 0:
        out, pad = rest
        b_at, out_at = 0, 0
    else:
        first_out, out, pad = rest
        b_at, out_at = 4, 1
        out[:, 0:1] = first_out[...]
    mask = has_partner()
    near = side()
    place = (near, 1 - near)
    height = inv.shape[1]
    strip = out.shape[3]
    own = ((own_a, 0), (own_b, 0 if p == 0 else b_at))
    got = ((got_a, 0), (got_b, b_at))
    med = ((med_a, 4), (got_b1, 4))
    clear_edges(pad)
    for layer in range(2):
        (mine, at), (theirs, from_) = own[layer], got[layer]
        for r, n in chunks(height):
            third = add(
                load(mine, at + 2, r, n),
                multiply_conj(load(inv, 2 * layer, r, n), load(theirs, from_, r, n)),
            )
            store(pad, 2 * layer, TOP + r, n, third)
    for layer in range(2):
        (mine, at), (theirs, from_) = own[layer], got[layer]
        for r, n in chunks(height):
            there = halo_inverse(med[layer][0][med[layer][1], r : r + n], layer, row, mask)
            halo = add(
                load(theirs, from_ + 2, r, n), multiply_conj(there, load(mine, at, r, n))
            )
            here, around = complex_in_plane(pad, layer, r, n)
            around = add(add(around, halo), load(pad, 2 * (1 - layer), TOP + r, n))
            fourth = add(
                add(scale(KEEP, here), load(right, 2 * layer, r, n)),
                multiply_conj(load(inv, 2 * layer, r, n), around),
            )
            wave = load(waves, 2 * layer, r, n)
            term = wave[0] * fourth[0] + wave[1] * fourth[1]
            for k in range(0, n, strip):
                out[(r + k) // strip, out_at, place[layer]] = term[k : k + strip]


def call(kernel, shapes, scratch, *args, space=pltpu.VMEM):
    vmem = pl.BlockSpec(memory_space=pltpu.VMEM)
    return pl.pallas_call(
        kernel,
        out_shape=[jax.ShapeDtypeStruct(s, jnp.float32) for s in shapes],
        in_specs=[pl.BlockSpec(memory_space=space)] * len(args),
        out_specs=[vmem] * len(shapes),
        scratch_shapes=scratch,
        cost_estimate=pl.CostEstimate(flops=2_000_000, bytes_accessed=2_000_000, transcendentals=0),
        compiler_params=pltpu.CompilerParams(vmem_limit_bytes=16 * 1024 * 1024),
    )(*args)


def swap_links(x):
    count = lax.axis_size("space")
    pairs = []
    for i in range(1, count - 1, 2):
        pairs += [(i, i + 1), (i + 1, i)]
    return lax.ppermute(x, "space", pairs)


def swap_cores(x):
    pairs = []
    for i in range(0, lax.axis_size("space"), 2):
        pairs += [(i, i + 1), (i + 1, i)]
    return lax.ppermute(x, "space", pairs)


def per_device(probes, background, medium, shifts, receivers):
    plane = medium.shape[1:]
    pad = pltpu.VMEM((4, plane[0] + 2 * TOP, plane[1]), jnp.float32)
    five, ten, four, eight = [(k, *plane) for k in (5, 10, 4, 8)]
    args = (shifts, background, probes, medium, receivers)
    held = [pltpu.VMEM(v.shape, v.dtype) for v in args[1:]]
    a1 = [None, None]
    a1[0], a1[1], b1, inv, waves, row = call(
        start_kernel,
        [five, five, ten, four, four, (2, 8, plane[1])],
        [pltpu.SMEM(shifts.shape, shifts.dtype), *held, pad, pltpu.SemaphoreType.DMA((5,))],
        *args,
        space=pltpu.HBM,
    )
    ra1 = [swap_links(a1[p]) for p in range(2)]
    rb1 = swap_cores(b1)
    a2, ra2, b2 = [None, None], [None, None], []
    for p in range(2):
        a2[p], out_b = call(
            functools.partial(forward_kernel, p),
            [four, eight if p else four],
            [pad, pad],
            row, a1[p], b1, ra1[p], rb1, ra1[0], inv, *b2,
        )
        b2.append(out_b)
        ra2[p] = swap_links(a2[p])
    rb2 = swap_cores(b2[1])
    a3, ra3, b3, right = [None, None], [None, None], [], [None, None]
    for p in range(2):
        a3[p], out_b, right[p] = call(
            functools.partial(turn_kernel, p),
            [four, eight if p else four, four],
            [pad, pad],
            row, a2[p], b2[p], ra2[p], rb2, ra1[0], rb1, ra1[1], a1[1], b1, inv, *b3,
        )
        b3.append(out_b)
        ra3[p] = swap_links(a3[p])
    rb3 = swap_cores(b3[1])
    blocks = lax.axis_size("freq")
    terms = []
    for p in range(2):
        (out,) = call(
            functools.partial(end_kernel, p),
            [(blocks, p + 1, 2, plane[0] // blocks, plane[1])],
            [pad],
            row, a3[p], b3[p], ra3[p], rb3, ra1[0], rb1, inv, right[p], waves, *terms,
        )
        terms.append(out)
    arrived = lax.all_to_all(terms[1], "freq", split_axis=0, concat_axis=0, tiled=True)
    return arrived.sum(axis=0)


def solution(mesh):
    in_specs = (
        P(None, "space", None, None),
        P("freq", None, "space", None, None),
        P("space", None, None),
        P("freq", None),
        P("space", None, None),
    )
    out_specs = P(None, "space", "freq", None)
    return jax.shard_map(
        per_device, mesh=mesh, in_specs=in_specs, out_specs=out_specs, check_vma=False
    )
```

```python
import functools

import jax
import jax.numpy as jnp
from jax import lax
from jax.experimental import pallas as pl
from jax.experimental.pallas import tpu as pltpu
from jax.sharding import PartitionSpec as P


OMEGA = 0.8
KEEP = 1.0 - OMEGA
TOP = 8
ROWS = 32


def multiply(x, y):
    return (x[0] * y[0] - x[1] * y[1], x[0] * y[1] + x[1] * y[0])


def multiply_conj(x, y):
    return (x[0] * y[0] + x[1] * y[1], x[0] * y[1] - x[1] * y[0])


def inverse(medium, shift_re, shift_im):
    diag_re = 6.0 + shift_re * medium
    diag_im = shift_im * medium
    scale = OMEGA / (diag_re * diag_re + diag_im * diag_im)
    return (diag_re * scale, -diag_im * scale)


def chunks(height):
    return [(r, min(ROWS, height - r)) for r in range(0, height, ROWS)]


def clear_edges(pad):
    height = pad.shape[-2] - 2 * TOP
    zero = jnp.zeros((TOP, pad.shape[-1]), jnp.float32)
    for part in range(pad.shape[0]):
        pad[part, 0:TOP] = zero
        pad[part, TOP + height :] = zero


def in_plane(pad, part, r, n):
    here = pad[part, TOP + r : TOP + r + n]
    width = here.shape[-1]
    lane = lax.broadcasted_iota(jnp.int32, here.shape, 1)
    left = jnp.where(lane == 0, 0.0, pltpu.roll(here, 1, 1))
    right = jnp.where(lane == width - 1, 0.0, pltpu.roll(here, width - 1, 1))
    above = pad[part, TOP + r - 1 : TOP + r - 1 + n]
    below = pad[part, TOP + r + 1 : TOP + r + 1 + n]
    return here, (left + right) + (above + below)


def complex_in_plane(pad, layer, r, n):
    re, sum_re = in_plane(pad, 2 * layer, r, n)
    im, sum_im = in_plane(pad, 2 * layer + 1, r, n)
    return (re, im), (sum_re, sum_im)


def store(ref, at, r, n, value):
    ref[at, r : r + n] = value[0]
    ref[at + 1, r : r + n] = value[1]


def load(ref, at, r, n):
    return (ref[at, r : r + n], ref[at + 1, r : r + n])


def add(x, y):
    return (x[0] + y[0], x[1] + y[1])


def scale(a, x):
    return (a * x[0], a * x[1])


def side():
    return lax.rem(lax.axis_index("space"), 2)


def has_partner():
    at = lax.axis_index("space")
    last = lax.axis_size("space") - 1
    return jnp.where((at == 0) | (at == last), 0.0, 1.0).astype(jnp.float32)


def start_kernel(
    shifts_hbm, back_hbm, probes_hbm, medium_hbm, receivers_hbm,
    out_a0, out_a1, out_b, inv, waves, row,
    shifts, back, probes, medium, receivers, pad, sems,
):
    copies = [
        pltpu.make_async_copy(src, dst, sems.at[k])
        for k, (src, dst) in enumerate(
            (
                (shifts_hbm, shifts),
                (medium_hbm, medium),
                (back_hbm, back),
                (probes_hbm, probes),
                (receivers_hbm, receivers),
            )
        )
    ]
    for copy in copies:
        copy.start()
    near = side()
    own = (near, 1 - near)
    height = medium.shape[1]
    outs = ((out_a0, 0), (out_a1, 0)), ((out_b, 0), (out_b, 5))
    clear_edges(pad)
    copies[0].wait()
    shift_re, shift_im = shifts[0, 0], shifts[0, 1]
    row[0] = jnp.full(row.shape[1:], shift_re, jnp.float32)
    row[1] = jnp.full(row.shape[1:], shift_im, jnp.float32)
    copies[1].wait()
    for layer in range(2):
        for r, n in chunks(height):
            med = medium[own[layer], r : r + n]
            store(inv, 2 * layer, r, n, inverse(med, shift_re, shift_im))
            outs[layer][0][0][outs[layer][0][1] + 4, r : r + n] = med
    copies[2].wait()
    for layer in range(2):
        for r, n in chunks(height):
            rows = slice(r, r + n)
            bg = (back[0, 0, own[layer], rows], back[0, 1, own[layer], rows])
            store(waves, 2 * layer, r, n, multiply((shift_re, shift_im), bg))
    copies[3].wait()
    for p in range(2):
        for layer in range(2):
            ref, at = outs[layer][p]
            for r, n in chunks(height):
                probe = probes[p, own[layer], r : r + n]
                first = scale(probe, multiply(load(inv, 2 * layer, r, n), load(waves, 2 * layer, r, n)))
                store(ref, at, r, n, first)
                store(pad, 2 * layer, TOP + r, n, first)
        for layer in range(2):
            ref, at = outs[layer][p]
            for r, n in chunks(height):
                here, around = complex_in_plane(pad, layer, r, n)
                around = add(around, load(pad, 2 * (1 - layer), TOP + r, n))
                part = add(scale(1.0 + KEEP, here), multiply(load(inv, 2 * layer, r, n), around))
                store(ref, at + 2, r, n, part)
    copies[4].wait()
    for layer in range(2):
        ref, at = outs[layer][1]
        for r, n in chunks(height):
            ref[at + 4, r : r + n] = receivers[own[layer], r : r + n].astype(jnp.float32)


def halo_inverse(med, layer, row, mask):
    re, im = inverse(med, row[0, 0:1], row[1, 0:1])
    return (mask * re, mask * im) if layer == 0 else (re, im)


def forward_kernel(p, row, own_a, own_b, got_a, got_b, med_a, inv, *rest):
    if p == 0:
        out_a, out_b, pad, spare = rest
        b_at, out_at = 0, 0
    else:
        first_b, out_a, out_b, pad, spare = rest
        b_at, out_at = 5, 4
        out_b[0:4] = first_b[...]
    mask = has_partner()
    height = inv.shape[1]
    own = ((own_a, 0), (own_b, b_at))
    got = ((got_a, 0), (got_b, b_at))
    med = ((med_a, 4), (got_b, 4))
    out = ((out_a, 0), (out_b, out_at))
    clear_edges(pad)
    clear_edges(spare)
    for layer in range(2):
        (mine, at), (theirs, from_) = own[layer], got[layer]
        for r, n in chunks(height):
            second = add(
                load(mine, at + 2, r, n),
                multiply(load(inv, 2 * layer, r, n), load(theirs, from_, r, n)),
            )
            store(pad, 2 * layer, TOP + r, n, second)
    for layer in range(2):
        (mine, at), (theirs, from_) = own[layer], got[layer]
        for r, n in chunks(height):
            first = load(mine, at, r, n)
            there = halo_inverse(med[layer][0][med[layer][1], r : r + n], layer, row, mask)
            halo = add(load(theirs, from_ + 2, r, n), multiply(there, first))
            here, around = complex_in_plane(pad, layer, r, n)
            around = add(add(around, halo), load(pad, 2 * (1 - layer), TOP + r, n))
            third = add(
                add(scale(KEEP, here), first), multiply(load(inv, 2 * layer, r, n), around)
            )
            store(spare, 2 * layer, TOP + r, n, third)
            store(out[layer][0], out[layer][1], r, n, third)
    for layer in range(2):
        mine, at = own[layer]
        for r, n in chunks(height):
            here, around = complex_in_plane(spare, layer, r, n)
            around = add(around, load(spare, 2 * (1 - layer), TOP + r, n))
            part = add(
                add(scale(KEEP, here), load(mine, at, r, n)),
                multiply(load(inv, 2 * layer, r, n), around),
            )
            store(out[layer][0], out[layer][1] + 2, r, n, part)


def turn_kernel(
    p, row, own_a, own_b, got_a, got_b, med_a, got_b1, rec_a, own_a1, own_b1, inv, *rest
):
    if p == 0:
        out_a, out_b, right, pad, spare = rest
        b_at, out_at = 0, 0
    else:
        first_b, out_a, out_b, right, pad, spare = rest
        b_at, out_at = 4, 4
        out_b[0:4] = first_b[...]
    mask = has_partner()
    height = inv.shape[1]
    own = ((own_a, 0), (own_b, 0 if p == 0 else b_at))
    got = ((got_a, 0), (got_b, b_at))
    med = ((med_a, 4), (got_b1, 4))
    rec_own = ((own_a1, 4), (own_b1, 9))
    rec_got = ((rec_a, 4), (got_b1, 9))
    out = ((out_a, 0), (out_b, out_at))
    clear_edges(pad)
    clear_edges(spare)
    for layer in range(2):
        (mine, at), (theirs, from_) = own[layer], got[layer]
        for r, n in chunks(height):
            there = load(inv, 2 * layer, r, n)
            fourth = add(load(mine, at + 2, r, n), multiply(there, load(theirs, from_, r, n)))
            heard = scale(rec_own[layer][0][rec_own[layer][1], r : r + n], fourth)
            first = multiply_conj(there, heard)
            store(pad, 2 * layer, TOP + r, n, first)
            store(right, 2 * layer, r, n, first)
    for layer in range(2):
        (mine, at), (theirs, from_) = own[layer], got[layer]
        for r, n in chunks(height):
            there = halo_inverse(med[layer][0][med[layer][1], r : r + n], layer, row, mask)
            fourth = add(load(theirs, from_ + 2, r, n), multiply(there, load(mine, at, r, n)))
            halo = multiply_conj(
                there, scale(rec_got[layer][0][rec_got[layer][1], r : r + n], fourth)
            )
            here, around = complex_in_plane(pad, layer, r, n)
            around = add(add(around, halo), load(pad, 2 * (1 - layer), TOP + r, n))
            second = add(
                scale(1.0 + KEEP, here), multiply_conj(load(inv, 2 * layer, r, n), around)
            )
            store(spare, 2 * layer, TOP + r, n, second)
            store(out[layer][0], out[layer][1], r, n, second)
    for layer in range(2):
        for r, n in chunks(height):
            here, around = complex_in_plane(spare, layer, r, n)
            around = add(around, load(spare, 2 * (1 - layer), TOP + r, n))
            part = add(
                add(scale(KEEP, here), load(right, 2 * layer, r, n)),
                multiply_conj(load(inv, 2 * layer, r, n), around),
            )
            store(out[layer][0], out[layer][1] + 2, r, n, part)


def end_kernel(p, row, own_a, own_b, got_a, got_b, med_a, got_b1, inv, right, waves, *rest):
    if p == 0:
        out, pad = rest
        b_at, out_at = 0, 0
    else:
        first_out, out, pad = rest
        b_at, out_at = 4, 1
        out[:, 0:1] = first_out[...]
    mask = has_partner()
    near = side()
    place = (near, 1 - near)
    height = inv.shape[1]
    strip = out.shape[3]
    own = ((own_a, 0), (own_b, 0 if p == 0 else b_at))
    got = ((got_a, 0), (got_b, b_at))
    med = ((med_a, 4), (got_b1, 4))
    clear_edges(pad)
    for layer in range(2):
        (mine, at), (theirs, from_) = own[layer], got[layer]
        for r, n in chunks(height):
            third = add(
                load(mine, at + 2, r, n),
                multiply_conj(load(inv, 2 * layer, r, n), load(theirs, from_, r, n)),
            )
            store(pad, 2 * layer, TOP + r, n, third)
    for layer in range(2):
        (mine, at), (theirs, from_) = own[layer], got[layer]
        for r, n in chunks(height):
            there = halo_inverse(med[layer][0][med[layer][1], r : r + n], layer, row, mask)
            halo = add(
                load(theirs, from_ + 2, r, n), multiply_conj(there, load(mine, at, r, n))
            )
            here, around = complex_in_plane(pad, layer, r, n)
            around = add(add(around, halo), load(pad, 2 * (1 - layer), TOP + r, n))
            fourth = add(
                add(scale(KEEP, here), load(right, 2 * layer, r, n)),
                multiply_conj(load(inv, 2 * layer, r, n), around),
            )
            wave = load(waves, 2 * layer, r, n)
            term = wave[0] * fourth[0] + wave[1] * fourth[1]
            for k in range(0, n, strip):
                out[(r + k) // strip, out_at, place[layer]] = term[k : k + strip]


def call(kernel, shapes, scratch, *args, space=pltpu.VMEM):
    vmem = pl.BlockSpec(memory_space=pltpu.VMEM)
    return pl.pallas_call(
        kernel,
        out_shape=[jax.ShapeDtypeStruct(s, jnp.float32) for s in shapes],
        in_specs=[pl.BlockSpec(memory_space=space)] * len(args),
        out_specs=[vmem] * len(shapes),
        scratch_shapes=scratch,
        cost_estimate=pl.CostEstimate(flops=2_000_000, bytes_accessed=2_000_000, transcendentals=0),
        compiler_params=pltpu.CompilerParams(vmem_limit_bytes=16 * 1024 * 1024),
    )(*args)


def swap_links(x):
    count = lax.axis_size("space")
    pairs = []
    for i in range(1, count - 1, 2):
        pairs += [(i, i + 1), (i + 1, i)]
    return lax.ppermute(x, "space", pairs)


def swap_cores(x):
    pairs = []
    for i in range(0, lax.axis_size("space"), 2):
        pairs += [(i, i + 1), (i + 1, i)]
    return lax.ppermute(x, "space", pairs)


def halves_kernel(arrived, keep, send):
    half = lax.rem(lax.axis_index("freq"), 2)
    count = arrived.shape[0] // 2
    for out, at in ((keep, half), (send, 1 - half)):
        for p in range(arrived.shape[1]):
            for layer in range(arrived.shape[2]):
                total = arrived[at, p, layer]
                for k in range(1, count):
                    total = total + arrived[2 * k + at, p, layer]
                out[p, layer] = total


def reduced(terms):
    count = lax.axis_size("freq")
    groups = [list(range(k, count, 2)) for k in range(2)]
    arrived = lax.all_to_all(
        terms, "freq", split_axis=0, concat_axis=0, axis_index_groups=groups, tiled=True
    )
    shape = terms.shape[1:]
    keep, send = call(halves_kernel, [shape, shape], [], arrived)
    pairs = [(k, k ^ 1) for k in range(count)]
    return keep + lax.ppermute(send, "freq", pairs)


def per_device(probes, background, medium, shifts, receivers):
    plane = medium.shape[1:]
    pad = pltpu.VMEM((4, plane[0] + 2 * TOP, plane[1]), jnp.float32)
    five, ten, four, eight = [(k, *plane) for k in (5, 10, 4, 8)]
    args = (shifts, background, probes, medium, receivers)
    held = [pltpu.VMEM(v.shape, v.dtype) for v in args[1:]]
    a1 = [None, None]
    a1[0], a1[1], b1, inv, waves, row = call(
        start_kernel,
        [five, five, ten, four, four, (2, 8, plane[1])],
        [pltpu.SMEM(shifts.shape, shifts.dtype), *held, pad, pltpu.SemaphoreType.DMA((5,))],
        *[pltpu.with_memory_space_constraint(v, pltpu.HBM) for v in args],
        space=pltpu.HBM,
    )
    ra1 = [swap_links(a1[p]) for p in range(2)]
    rb1 = swap_cores(b1)
    a2, ra2, b2 = [None, None], [None, None], []
    for p in range(2):
        a2[p], out_b = call(
            functools.partial(forward_kernel, p),
            [four, eight if p else four],
            [pad, pad],
            row, a1[p], b1, ra1[p], rb1, ra1[0], inv, *b2,
        )
        b2.append(out_b)
        ra2[p] = swap_links(a2[p])
    rb2 = swap_cores(b2[1])
    a3, ra3, b3, right = [None, None], [None, None], [], [None, None]
    for p in range(2):
        a3[p], out_b, right[p] = call(
            functools.partial(turn_kernel, p),
            [four, eight if p else four, four],
            [pad, pad],
            row, a2[p], b2[p], ra2[p], rb2, ra1[0], rb1, ra1[1], a1[1], b1, inv, *b3,
        )
        b3.append(out_b)
        ra3[p] = swap_links(a3[p])
    rb3 = swap_cores(b3[1])
    blocks = lax.axis_size("freq")
    terms = []
    for p in range(2):
        (out,) = call(
            functools.partial(end_kernel, p),
            [(blocks, p + 1, 2, plane[0] // blocks, plane[1])],
            [pad],
            row, a3[p], b3[p], ra3[p], rb3, ra1[0], rb1, inv, right[p], waves, *terms,
        )
        terms.append(out)
    return reduced(terms[1])


def solution(mesh):
    in_specs = (
        P(None, "space", None, None),
        P("freq", None, "space", None, None),
        P("space", None, None),
        P("freq", None),
        P("space", None, None),
    )
    out_specs = P(None, "space", "freq", None)
    return jax.shard_map(
        per_device, mesh=mesh, in_specs=in_specs, out_specs=out_specs, check_vma=False
    )
```

```python
import functools

import jax
import jax.numpy as jnp
from jax import lax
from jax.experimental import pallas as pl
from jax.experimental.pallas import tpu as pltpu
from jax.sharding import PartitionSpec as P


OMEGA = 0.8
KEEP = 1.0 - OMEGA
TOP = 8
ROWS = 32


def multiply(x, y):
    return (x[0] * y[0] - x[1] * y[1], x[0] * y[1] + x[1] * y[0])


def multiply_conj(x, y):
    return (x[0] * y[0] + x[1] * y[1], x[0] * y[1] - x[1] * y[0])


def inverse(medium, shift_re, shift_im):
    diag_re = 6.0 + shift_re * medium
    diag_im = shift_im * medium
    scale = OMEGA / (diag_re * diag_re + diag_im * diag_im)
    return (diag_re * scale, -diag_im * scale)


def chunks(height):
    return [(r, min(ROWS, height - r)) for r in range(0, height, ROWS)]


def clear_edges(pad):
    height = pad.shape[-2] - 2 * TOP
    zero = jnp.zeros((TOP, pad.shape[-1]), jnp.float32)
    for part in range(pad.shape[0]):
        pad[part, 0:TOP] = zero
        pad[part, TOP + height :] = zero


def in_plane(pad, part, r, n):
    here = pad[part, TOP + r : TOP + r + n]
    width = here.shape[-1]
    lane = lax.broadcasted_iota(jnp.int32, here.shape, 1)
    left = jnp.where(lane == 0, 0.0, pltpu.roll(here, 1, 1))
    right = jnp.where(lane == width - 1, 0.0, pltpu.roll(here, width - 1, 1))
    above = pad[part, TOP + r - 1 : TOP + r - 1 + n]
    below = pad[part, TOP + r + 1 : TOP + r + 1 + n]
    return here, (left + right) + (above + below)


def complex_in_plane(pad, layer, r, n):
    re, sum_re = in_plane(pad, 2 * layer, r, n)
    im, sum_im = in_plane(pad, 2 * layer + 1, r, n)
    return (re, im), (sum_re, sum_im)


def store(ref, at, r, n, value):
    ref[at, r : r + n] = value[0]
    ref[at + 1, r : r + n] = value[1]


def load(ref, at, r, n):
    return (ref[at, r : r + n], ref[at + 1, r : r + n])


def add(x, y):
    return (x[0] + y[0], x[1] + y[1])


def scale(a, x):
    return (a * x[0], a * x[1])


def side():
    return lax.rem(lax.axis_index("space"), 2)


def has_partner():
    at = lax.axis_index("space")
    last = lax.axis_size("space") - 1
    return jnp.where((at == 0) | (at == last), 0.0, 1.0).astype(jnp.float32)


def probe_at(parts, p):
    ref, at = parts[p]
    return (ref, at + 2) if p == 0 else (ref, at)


def first_of(parts, p, r, n):
    (gain, gain_at), (ref, at) = parts[0], probe_at(parts, p)
    return scale(ref[at, r : r + n], load(gain, gain_at, r, n))


def start_kernel(
    shifts_hbm, back_hbm, probes_hbm, medium_hbm, receivers_hbm,
    out_a0, out_a1, out_b, inv, waves, row,
    shifts, back, probes, medium, receivers, pad, sems,
):
    copies = [
        pltpu.make_async_copy(src, dst, sems.at[k])
        for k, (src, dst) in enumerate(
            (
                (shifts_hbm, shifts),
                (medium_hbm, medium),
                (back_hbm, back),
                (probes_hbm, probes),
                (receivers_hbm, receivers),
            )
        )
    ]
    for copy in copies:
        copy.start()
    near = side()
    own = (near, 1 - near)
    height = medium.shape[1]
    outs = ((out_a0, 0), (out_a1, 0)), ((out_b, 0), (out_b, 6))
    clear_edges(pad)
    copies[0].wait()
    shift_re, shift_im = shifts[0, 0], shifts[0, 1]
    row[0] = jnp.full(row.shape[1:], shift_re, jnp.float32)
    row[1] = jnp.full(row.shape[1:], shift_im, jnp.float32)
    copies[1].wait()
    for layer in range(2):
        for r, n in chunks(height):
            med = medium[own[layer], r : r + n]
            store(inv, 2 * layer, r, n, inverse(med, shift_re, shift_im))
            outs[layer][0][0][outs[layer][0][1] + 5, r : r + n] = med
    copies[2].wait()
    for layer in range(2):
        ref, at = outs[layer][0]
        for r, n in chunks(height):
            rows = slice(r, r + n)
            bg = (back[0, 0, own[layer], rows], back[0, 1, own[layer], rows])
            wave = multiply((shift_re, shift_im), bg)
            store(waves, 2 * layer, r, n, wave)
            store(ref, at, r, n, multiply(load(inv, 2 * layer, r, n), wave))
    copies[3].wait()
    for p in range(2):
        for layer in range(2):
            gain, gain_at = outs[layer][0]
            ref, at = probe_at(outs[layer], p)
            for r, n in chunks(height):
                probe = probes[p, own[layer], r : r + n]
                ref[at, r : r + n] = probe
                store(pad, 2 * layer, TOP + r, n, scale(probe, load(gain, gain_at, r, n)))
        for layer in range(2):
            ref, at = probe_at(outs[layer], p)
            for r, n in chunks(height):
                here, around = complex_in_plane(pad, layer, r, n)
                around = add(around, load(pad, 2 * (1 - layer), TOP + r, n))
                part = add(scale(1.0 + KEEP, here), multiply(load(inv, 2 * layer, r, n), around))
                store(ref, at + 1, r, n, part)
    copies[4].wait()
    for layer in range(2):
        ref, at = outs[layer][1]
        for r, n in chunks(height):
            ref[at + 3, r : r + n] = receivers[own[layer], r : r + n].astype(jnp.float32)


def halo_inverse(med, layer, row, mask):
    re, im = inverse(med, row[0, 0:1], row[1, 0:1])
    return (mask * re, mask * im) if layer == 0 else (re, im)


def forward_kernel(p, row, own_a0, own_a, own_b, got_a0, got_a, got_b, inv, *rest):
    if p == 0:
        out_a, out_b, pad, spare = rest
        out_at = 0
    else:
        first_b, out_a, out_b, pad, spare = rest
        out_at = 4
        out_b[0:4] = first_b[...]
    mask = has_partner()
    height = inv.shape[1]
    own = ((own_a0, 0), (own_a, 0)), ((own_b, 0), (own_b, 6))
    got = ((got_a0, 0), (got_a, 0)), ((got_b, 0), (got_b, 6))
    out = ((out_a, 0), (out_b, out_at))
    clear_edges(pad)
    clear_edges(spare)
    for layer in range(2):
        mine, at = probe_at(own[layer], p)
        for r, n in chunks(height):
            second = add(
                load(mine, at + 1, r, n),
                multiply(load(inv, 2 * layer, r, n), first_of(got[layer], p, r, n)),
            )
            store(pad, 2 * layer, TOP + r, n, second)
    for layer in range(2):
        theirs, from_ = probe_at(got[layer], p)
        med, med_at = got[layer][0]
        for r, n in chunks(height):
            first = first_of(own[layer], p, r, n)
            there = halo_inverse(med[med_at + 5, r : r + n], layer, row, mask)
            halo = add(load(theirs, from_ + 1, r, n), multiply(there, first))
            here, around = complex_in_plane(pad, layer, r, n)
            around = add(add(around, halo), load(pad, 2 * (1 - layer), TOP + r, n))
            third = add(
                add(scale(KEEP, here), first), multiply(load(inv, 2 * layer, r, n), around)
            )
            store(spare, 2 * layer, TOP + r, n, third)
            store(out[layer][0], out[layer][1], r, n, third)
    for layer in range(2):
        for r, n in chunks(height):
            here, around = complex_in_plane(spare, layer, r, n)
            around = add(around, load(spare, 2 * (1 - layer), TOP + r, n))
            part = add(
                add(scale(KEEP, here), first_of(own[layer], p, r, n)),
                multiply(load(inv, 2 * layer, r, n), around),
            )
            store(out[layer][0], out[layer][1] + 2, r, n, part)


def turn_kernel(
    p, row, own_a, own_b, got_a, got_b, med_a, got_b1, rec_a, own_a1, own_b1, inv, *rest
):
    if p == 0:
        out_a, out_b, right, part_sum, pad, spare = rest
        b_at, out_at = 0, 0
    else:
        first_b, out_a, out_b, right, part_sum, pad, spare = rest
        b_at, out_at = 4, 3
        out_b[0:3] = first_b[...]
    mask = has_partner()
    height = inv.shape[1]
    own = ((own_a, 0), (own_b, 0 if p == 0 else b_at))
    got = ((got_a, 0), (got_b, b_at))
    med = ((med_a, 5), (got_b1, 5))
    rec_own = ((own_a1, 3), (own_b1, 9))
    rec_got = ((rec_a, 3), (got_b1, 9))
    gain = (med_a, got_b1)
    out = ((out_a, 0), (out_b, out_at))
    clear_edges(pad)
    clear_edges(spare)
    for layer in range(2):
        (mine, at), (theirs, from_) = own[layer], got[layer]
        for r, n in chunks(height):
            there = load(inv, 2 * layer, r, n)
            fourth = add(load(mine, at + 2, r, n), multiply(there, load(theirs, from_, r, n)))
            heard = scale(rec_own[layer][0][rec_own[layer][1], r : r + n], fourth)
            first = multiply_conj(there, heard)
            store(pad, 2 * layer, TOP + r, n, first)
            store(right, 2 * layer, r, n, first)
    for layer in range(2):
        (mine, at), (theirs, from_) = own[layer], got[layer]
        for r, n in chunks(height):
            there = halo_inverse(med[layer][0][med[layer][1], r : r + n], layer, row, mask)
            fourth = add(load(theirs, from_ + 2, r, n), multiply(there, load(mine, at, r, n)))
            halo = multiply_conj(
                there, scale(rec_got[layer][0][rec_got[layer][1], r : r + n], fourth)
            )
            here, around = complex_in_plane(pad, layer, r, n)
            around = add(add(around, halo), load(pad, 2 * (1 - layer), TOP + r, n))
            second = add(
                scale(1.0 + KEEP, here), multiply_conj(load(inv, 2 * layer, r, n), around)
            )
            store(spare, 2 * layer, TOP + r, n, second)
            store(out[layer][0], out[layer][1], r, n, second)
    for layer in range(2):
        for r, n in chunks(height):
            here, around = complex_in_plane(spare, layer, r, n)
            around = add(around, load(spare, 2 * (1 - layer), TOP + r, n))
            part = add(
                add(scale(KEEP, here), load(right, 2 * layer, r, n)),
                multiply_conj(load(inv, 2 * layer, r, n), around),
            )
            store(part_sum, 2 * layer, r, n, part)
            seen = load(gain[layer], 0, r, n)
            out[layer][0][out[layer][1] + 2, r : r + n] = seen[0] * part[0] + seen[1] * part[1]


def end_kernel(p, row, own_a, own_b, got_a, got_b, med_a, got_b1, inv, right, part_sum, waves, own_a1, own_b1, *rest):
    if p == 0:
        out, pad = rest
        b_at, out_at = 0, 0
    else:
        first_out, out, pad = rest
        b_at, out_at = 3, 1
        out[:, 0:1] = first_out[...]
    mask = has_partner()
    near = side()
    place = (near, 1 - near)
    height = inv.shape[1]
    strip = out.shape[3]
    own = ((own_a, 0), (own_b, 0 if p == 0 else b_at))
    got = ((got_a, 0), (got_b, b_at))
    med = ((med_a, 5), (got_b1, 5))
    gain = (own_a1, own_b1)
    clear_edges(pad)
    for layer in range(2):
        (mine, at), (theirs, from_) = own[layer], got[layer]
        for r, n in chunks(height):
            third = add(
                load(part_sum, 2 * layer, r, n),
                multiply_conj(load(inv, 2 * layer, r, n), load(theirs, from_, r, n)),
            )
            store(pad, 2 * layer, TOP + r, n, third)
    for layer in range(2):
        (mine, at), (theirs, from_) = own[layer], got[layer]
        for r, n in chunks(height):
            there = halo_inverse(med[layer][0][med[layer][1], r : r + n], layer, row, mask)
            halo = multiply_conj(there, load(mine, at, r, n))
            seen = load(gain[layer], 0, r, n)
            across = theirs[from_ + 2, r : r + n] + (seen[0] * halo[0] + seen[1] * halo[1])
            here, around = complex_in_plane(pad, layer, r, n)
            around = add(around, load(pad, 2 * (1 - layer), TOP + r, n))
            fourth = add(
                add(scale(KEEP, here), load(right, 2 * layer, r, n)),
                multiply_conj(load(inv, 2 * layer, r, n), around),
            )
            wave = load(waves, 2 * layer, r, n)
            term = (wave[0] * fourth[0] + wave[1] * fourth[1]) + across
            for k in range(0, n, strip):
                out[(r + k) // strip, out_at, place[layer]] = term[k : k + strip]


def call(kernel, shapes, scratch, *args, space=pltpu.VMEM):
    vmem = pl.BlockSpec(memory_space=pltpu.VMEM)
    return pl.pallas_call(
        kernel,
        out_shape=[jax.ShapeDtypeStruct(s, jnp.float32) for s in shapes],
        in_specs=[pl.BlockSpec(memory_space=space)] * len(args),
        out_specs=[vmem] * len(shapes),
        scratch_shapes=scratch,
        cost_estimate=pl.CostEstimate(flops=2_000_000, bytes_accessed=2_000_000, transcendentals=0),
        compiler_params=pltpu.CompilerParams(vmem_limit_bytes=16 * 1024 * 1024),
    )(*args)


def swap_links(x):
    count = lax.axis_size("space")
    pairs = []
    for i in range(1, count - 1, 2):
        pairs += [(i, i + 1), (i + 1, i)]
    return lax.ppermute(x, "space", pairs)


def swap_cores(x):
    pairs = []
    for i in range(0, lax.axis_size("space"), 2):
        pairs += [(i, i + 1), (i + 1, i)]
    return lax.ppermute(x, "space", pairs)


def halves_kernel(arrived, keep, send):
    half = lax.rem(lax.axis_index("freq"), 2)
    count = arrived.shape[0] // 2
    for out, at in ((keep, half), (send, 1 - half)):
        for p in range(arrived.shape[1]):
            for layer in range(arrived.shape[2]):
                total = arrived[at, p, layer]
                for k in range(1, count):
                    total = total + arrived[2 * k + at, p, layer]
                out[p, layer] = total


def reduced(terms):
    count = lax.axis_size("freq")
    groups = [list(range(k, count, 2)) for k in range(2)]
    arrived = lax.all_to_all(
        terms, "freq", split_axis=0, concat_axis=0, axis_index_groups=groups, tiled=True
    )
    shape = terms.shape[1:]
    keep, send = call(halves_kernel, [shape, shape], [], arrived)
    pairs = [(k, k ^ 1) for k in range(count)]
    return keep + lax.ppermute(send, "freq", pairs)


def per_device(probes, background, medium, shifts, receivers):
    plane = medium.shape[1:]
    pad = pltpu.VMEM((4, plane[0] + 2 * TOP, plane[1]), jnp.float32)
    three, four, six, eight, ten = [(k, *plane) for k in (3, 4, 6, 8, 10)]
    args = (shifts, background, probes, medium, receivers)
    held = [pltpu.VMEM(v.shape, v.dtype) for v in args[1:]]
    a1 = [None, None]
    a1[0], a1[1], b1, inv, waves, row = call(
        start_kernel,
        [six, four, ten, four, four, (2, 8, plane[1])],
        [pltpu.SMEM(shifts.shape, shifts.dtype), *held, pad, pltpu.SemaphoreType.DMA((5,))],
        *[pltpu.with_memory_space_constraint(v, pltpu.HBM) for v in args],
        space=pltpu.HBM,
    )
    ra1 = [swap_links(a1[p]) for p in range(2)]
    rb1 = swap_cores(b1)
    a2, ra2, b2 = [None, None], [None, None], []
    for p in range(2):
        a2[p], out_b = call(
            functools.partial(forward_kernel, p),
            [four, eight if p else four],
            [pad, pad],
            row, a1[0], a1[p], b1, ra1[0], ra1[p], rb1, inv, *b2,
        )
        b2.append(out_b)
        ra2[p] = swap_links(a2[p])
    rb2 = swap_cores(b2[1])
    a3, ra3, b3 = [None, None], [None, None], []
    right, part_sum = [None, None], [None, None]
    for p in range(2):
        a3[p], out_b, right[p], part_sum[p] = call(
            functools.partial(turn_kernel, p),
            [three, six if p else three, four, four],
            [pad, pad],
            row, a2[p], b2[p], ra2[p], rb2, ra1[0], rb1, ra1[1], a1[1], b1, inv, *b3,
        )
        b3.append(out_b)
        ra3[p] = swap_links(a3[p])
    rb3 = swap_cores(b3[1])
    blocks = lax.axis_size("freq")
    terms = []
    for p in range(2):
        (out,) = call(
            functools.partial(end_kernel, p),
            [(blocks, p + 1, 2, plane[0] // blocks, plane[1])],
            [pad],
            row, a3[p], b3[p], ra3[p], rb3, ra1[0], rb1, inv, right[p], part_sum[p],
            waves, a1[0], b1, *terms,
        )
        terms.append(out)
    return reduced(terms[1])


def solution(mesh):
    in_specs = (
        P(None, "space", None, None),
        P("freq", None, "space", None, None),
        P("space", None, None),
        P("freq", None),
        P("space", None, None),
    )
    out_specs = P(None, "space", "freq", None)
    return jax.shard_map(
        per_device, mesh=mesh, in_specs=in_specs, out_specs=out_specs, check_vma=False
    )
```

```python
import functools

import jax
import jax.numpy as jnp
from jax import lax
from jax.experimental import pallas as pl
from jax.experimental.pallas import tpu as pltpu
from jax.sharding import PartitionSpec as P


OMEGA = 0.8
KEEP = 1.0 - OMEGA
TOP = 8
ROWS = 32


def multiply(x, y):
    return (x[0] * y[0] - x[1] * y[1], x[0] * y[1] + x[1] * y[0])


def multiply_conj(x, y):
    return (x[0] * y[0] + x[1] * y[1], x[0] * y[1] - x[1] * y[0])


def inverse(medium, shift_re, shift_im):
    diag_re = 6.0 + shift_re * medium
    diag_im = shift_im * medium
    scale = OMEGA / (diag_re * diag_re + diag_im * diag_im)
    return (diag_re * scale, -diag_im * scale)


def chunks(height):
    return [(r, min(ROWS, height - r)) for r in range(0, height, ROWS)]


def clear_edges(pad):
    height = pad.shape[-2] - 2 * TOP
    zero = jnp.zeros((TOP, pad.shape[-1]), jnp.float32)
    for part in range(pad.shape[0]):
        pad[part, 0:TOP] = zero
        pad[part, TOP + height :] = zero


def in_plane(pad, part, r, n):
    here = pad[part, TOP + r : TOP + r + n]
    width = here.shape[-1]
    lane = lax.broadcasted_iota(jnp.int32, here.shape, 1)
    left = jnp.where(lane == 0, 0.0, pltpu.roll(here, 1, 1))
    right = jnp.where(lane == width - 1, 0.0, pltpu.roll(here, width - 1, 1))
    above = pad[part, TOP + r - 1 : TOP + r - 1 + n]
    below = pad[part, TOP + r + 1 : TOP + r + 1 + n]
    return here, (left + right) + (above + below)


def complex_in_plane(pad, layer, r, n):
    re, sum_re = in_plane(pad, 2 * layer, r, n)
    im, sum_im = in_plane(pad, 2 * layer + 1, r, n)
    return (re, im), (sum_re, sum_im)


def store(ref, at, r, n, value):
    ref[at, r : r + n] = value[0]
    ref[at + 1, r : r + n] = value[1]


def load(ref, at, r, n):
    return (ref[at, r : r + n], ref[at + 1, r : r + n])


def add(x, y):
    return (x[0] + y[0], x[1] + y[1])


def scale(a, x):
    return (a * x[0], a * x[1])


def side():
    return lax.rem(lax.axis_index("space"), 2)


def has_partner():
    at = lax.axis_index("space")
    last = lax.axis_size("space") - 1
    return jnp.where((at == 0) | (at == last), 0.0, 1.0).astype(jnp.float32)


def first_of(layer, parts, p, r, n):
    if layer == 0:
        return load(parts[p], 0, r, n)
    both = parts[2]
    return scale(both[2 + 4 * p, r : r + n], load(both, 0, r, n))


def partial_of(layer, parts, p, r, n):
    return load(parts[p], 2, r, n) if layer == 0 else load(parts[2], 3 + 4 * p, r, n)


def start_kernel(
    shifts_hbm, back_hbm, probes_hbm, medium_hbm, receivers_hbm,
    out_a0, out_a1, out_b, later, inv, waves, row,
    shifts, back, probes, medium, receivers, pad, sems,
):
    copies = [
        pltpu.make_async_copy(src, dst, sems.at[k])
        for k, (src, dst) in enumerate(
            (
                (shifts_hbm, shifts),
                (medium_hbm, medium),
                (back_hbm, back),
                (probes_hbm, probes),
                (receivers_hbm, receivers),
            )
        )
    ]
    for copy in copies:
        copy.start()
    near = side()
    own = (near, 1 - near)
    height = medium.shape[1]
    medium_at = ((out_a0, 4), (out_b, 5))
    gain_at = ((later, 0), (out_b, 0))
    heard_at = ((later, 2), (out_b, 9))
    clear_edges(pad)
    copies[0].wait()
    shift_re, shift_im = shifts[0, 0], shifts[0, 1]
    row[0] = jnp.full(row.shape[1:], shift_re, jnp.float32)
    row[1] = jnp.full(row.shape[1:], shift_im, jnp.float32)
    copies[1].wait()
    for layer in range(2):
        ref, at = medium_at[layer]
        for r, n in chunks(height):
            med = medium[own[layer], r : r + n]
            store(inv, 2 * layer, r, n, inverse(med, shift_re, shift_im))
            ref[at, r : r + n] = med
    copies[2].wait()
    for layer in range(2):
        ref, at = gain_at[layer]
        for r, n in chunks(height):
            rows = slice(r, r + n)
            bg = (back[0, 0, own[layer], rows], back[0, 1, own[layer], rows])
            wave = multiply((shift_re, shift_im), bg)
            store(waves, 2 * layer, r, n, wave)
            store(ref, at, r, n, multiply(load(inv, 2 * layer, r, n), wave))
    copies[3].wait()
    for p in range(2):
        link = (out_a0, out_a1)[p]
        for layer in range(2):
            gain, at = gain_at[layer]
            for r, n in chunks(height):
                probe = probes[p, own[layer], r : r + n]
                first = scale(probe, load(gain, at, r, n))
                store(pad, 2 * layer, TOP + r, n, first)
                if layer == 0:
                    store(link, 0, r, n, first)
                else:
                    out_b[2 + 4 * p, r : r + n] = probe
        for layer in range(2):
            ref, at = ((link, 2), (out_b, 3 + 4 * p))[layer]
            for r, n in chunks(height):
                here, around = complex_in_plane(pad, layer, r, n)
                around = add(around, load(pad, 2 * (1 - layer), TOP + r, n))
                part = add(scale(1.0 + KEEP, here), multiply(load(inv, 2 * layer, r, n), around))
                store(ref, at, r, n, part)
    copies[4].wait()
    for layer in range(2):
        ref, at = heard_at[layer]
        for r, n in chunks(height):
            ref[at, r : r + n] = receivers[own[layer], r : r + n].astype(jnp.float32)


def halo_inverse(med, layer, row, mask):
    re, im = inverse(med, row[0, 0:1], row[1, 0:1])
    return (mask * re, mask * im) if layer == 0 else (re, im)


def forward_kernel(
    p, row, own_a0, own_a1, own_b, got_a0, got_a1, got_b, inv, extra, *rest
):
    height = inv.shape[1]
    if p == 0:
        out_a, out_b, pad, spare = rest
        out_at = 0
        for k in range(extra.shape[0]):
            for r, n in chunks(height):
                out_a[4 + k, r : r + n] = extra[k, r : r + n]
    else:
        out_a, out_b, pad, spare = rest
        out_at = 4
        out_b[0:4] = extra[...]
    mask = has_partner()
    own = (own_a0, own_a1, own_b)
    got = (got_a0, got_a1, got_b)
    med = ((got_a0, 4), (got_b, 5))
    out = ((out_a, 0), (out_b, out_at))
    clear_edges(pad)
    clear_edges(spare)
    for layer in range(2):
        for r, n in chunks(height):
            second = add(
                partial_of(layer, own, p, r, n),
                multiply(load(inv, 2 * layer, r, n), first_of(layer, got, p, r, n)),
            )
            store(pad, 2 * layer, TOP + r, n, second)
    for layer in range(2):
        for r, n in chunks(height):
            first = first_of(layer, own, p, r, n)
            there = halo_inverse(med[layer][0][med[layer][1], r : r + n], layer, row, mask)
            halo = add(partial_of(layer, got, p, r, n), multiply(there, first))
            here, around = complex_in_plane(pad, layer, r, n)
            around = add(add(around, halo), load(pad, 2 * (1 - layer), TOP + r, n))
            third = add(
                add(scale(KEEP, here), first), multiply(load(inv, 2 * layer, r, n), around)
            )
            store(spare, 2 * layer, TOP + r, n, third)
            store(out[layer][0], out[layer][1], r, n, third)
    for layer in range(2):
        for r, n in chunks(height):
            here, around = complex_in_plane(spare, layer, r, n)
            around = add(around, load(spare, 2 * (1 - layer), TOP + r, n))
            part = add(
                add(scale(KEEP, here), first_of(layer, own, p, r, n)),
                multiply(load(inv, 2 * layer, r, n), around),
            )
            store(out[layer][0], out[layer][1] + 2, r, n, part)


def turn_kernel(
    p, row, own_a, own_b, got_a, got_b, med_a, got_a2, got_b1, later, own_b1, inv, *rest
):
    if p == 0:
        out_a, out_b, right, part_sum, pad, spare = rest
        b_at, out_at = 0, 0
    else:
        first_b, out_a, out_b, right, part_sum, pad, spare = rest
        b_at, out_at = 4, 3
        out_b[0:3] = first_b[...]
    mask = has_partner()
    height = inv.shape[1]
    own = ((own_a, 0), (own_b, 0 if p == 0 else b_at))
    got = ((got_a, 0), (got_b, b_at))
    med = ((med_a, 4), (got_b1, 5))
    rec_own = ((later, 2), (own_b1, 9))
    rec_got = ((got_a2, 6), (got_b1, 9))
    gain = ((got_a2, 4), (got_b1, 0))
    out = ((out_a, 0), (out_b, out_at))
    clear_edges(pad)
    clear_edges(spare)
    for layer in range(2):
        (mine, at), (theirs, from_) = own[layer], got[layer]
        for r, n in chunks(height):
            there = load(inv, 2 * layer, r, n)
            fourth = add(load(mine, at + 2, r, n), multiply(there, load(theirs, from_, r, n)))
            heard = scale(rec_own[layer][0][rec_own[layer][1], r : r + n], fourth)
            first = multiply_conj(there, heard)
            store(pad, 2 * layer, TOP + r, n, first)
            store(right, 2 * layer, r, n, first)
    for layer in range(2):
        (mine, at), (theirs, from_) = own[layer], got[layer]
        for r, n in chunks(height):
            there = halo_inverse(med[layer][0][med[layer][1], r : r + n], layer, row, mask)
            fourth = add(load(theirs, from_ + 2, r, n), multiply(there, load(mine, at, r, n)))
            halo = multiply_conj(
                there, scale(rec_got[layer][0][rec_got[layer][1], r : r + n], fourth)
            )
            here, around = complex_in_plane(pad, layer, r, n)
            around = add(add(around, halo), load(pad, 2 * (1 - layer), TOP + r, n))
            second = add(
                scale(1.0 + KEEP, here), multiply_conj(load(inv, 2 * layer, r, n), around)
            )
            store(spare, 2 * layer, TOP + r, n, second)
            store(out[layer][0], out[layer][1], r, n, second)
    for layer in range(2):
        for r, n in chunks(height):
            here, around = complex_in_plane(spare, layer, r, n)
            around = add(around, load(spare, 2 * (1 - layer), TOP + r, n))
            part = add(
                add(scale(KEEP, here), load(right, 2 * layer, r, n)),
                multiply_conj(load(inv, 2 * layer, r, n), around),
            )
            store(part_sum, 2 * layer, r, n, part)
            seen = load(*gain[layer], r, n)
            out[layer][0][out[layer][1] + 2, r : r + n] = seen[0] * part[0] + seen[1] * part[1]


def end_kernel(p, row, own_a, own_b, got_a, got_b, med_a, got_b1, inv, right, part_sum, waves, later, own_b1, *rest):
    if p == 0:
        out, pad = rest
        b_at, out_at = 0, 0
    else:
        first_out, out, pad = rest
        b_at, out_at = 3, 1
        out[:, 0:1] = first_out[...]
    mask = has_partner()
    near = side()
    place = (near, 1 - near)
    height = inv.shape[1]
    strip = out.shape[3]
    own = ((own_a, 0), (own_b, 0 if p == 0 else b_at))
    got = ((got_a, 0), (got_b, b_at))
    med = ((med_a, 4), (got_b1, 5))
    gain = (later, own_b1)
    clear_edges(pad)
    for layer in range(2):
        (mine, at), (theirs, from_) = own[layer], got[layer]
        for r, n in chunks(height):
            third = add(
                load(part_sum, 2 * layer, r, n),
                multiply_conj(load(inv, 2 * layer, r, n), load(theirs, from_, r, n)),
            )
            store(pad, 2 * layer, TOP + r, n, third)
    for layer in range(2):
        (mine, at), (theirs, from_) = own[layer], got[layer]
        for r, n in chunks(height):
            there = halo_inverse(med[layer][0][med[layer][1], r : r + n], layer, row, mask)
            halo = multiply_conj(there, load(mine, at, r, n))
            seen = load(gain[layer], 0, r, n)
            across = theirs[from_ + 2, r : r + n] + (seen[0] * halo[0] + seen[1] * halo[1])
            here, around = complex_in_plane(pad, layer, r, n)
            around = add(around, load(pad, 2 * (1 - layer), TOP + r, n))
            fourth = add(
                add(scale(KEEP, here), load(right, 2 * layer, r, n)),
                multiply_conj(load(inv, 2 * layer, r, n), around),
            )
            wave = load(waves, 2 * layer, r, n)
            term = (wave[0] * fourth[0] + wave[1] * fourth[1]) + across
            for k in range(0, n, strip):
                out[(r + k) // strip, out_at, place[layer]] = term[k : k + strip]


def call(kernel, shapes, scratch, *args, space=pltpu.VMEM):
    vmem = pl.BlockSpec(memory_space=pltpu.VMEM)
    return pl.pallas_call(
        kernel,
        out_shape=[jax.ShapeDtypeStruct(s, jnp.float32) for s in shapes],
        in_specs=[pl.BlockSpec(memory_space=space)] * len(args),
        out_specs=[vmem] * len(shapes),
        scratch_shapes=scratch,
        cost_estimate=pl.CostEstimate(flops=2_000_000, bytes_accessed=2_000_000, transcendentals=0),
        compiler_params=pltpu.CompilerParams(vmem_limit_bytes=16 * 1024 * 1024),
    )(*args)


def swap_links(x):
    count = lax.axis_size("space")
    pairs = []
    for i in range(1, count - 1, 2):
        pairs += [(i, i + 1), (i + 1, i)]
    return lax.ppermute(x, "space", pairs)


def swap_cores(x):
    pairs = []
    for i in range(0, lax.axis_size("space"), 2):
        pairs += [(i, i + 1), (i + 1, i)]
    return lax.ppermute(x, "space", pairs)


def halves_kernel(arrived, keep, send):
    half = lax.rem(lax.axis_index("freq"), 2)
    count = arrived.shape[0] // 2
    for out, at in ((keep, half), (send, 1 - half)):
        for p in range(arrived.shape[1]):
            for layer in range(arrived.shape[2]):
                total = arrived[at, p, layer]
                for k in range(1, count):
                    total = total + arrived[2 * k + at, p, layer]
                out[p, layer] = total


def reduced(terms):
    count = lax.axis_size("freq")
    groups = [list(range(k, count, 2)) for k in range(2)]
    arrived = lax.all_to_all(
        terms, "freq", split_axis=0, concat_axis=0, axis_index_groups=groups, tiled=True
    )
    shape = terms.shape[1:]
    keep, send = call(halves_kernel, [shape, shape], [], arrived)
    pairs = [(k, k ^ 1) for k in range(count)]
    return keep + lax.ppermute(send, "freq", pairs)


def per_device(probes, background, medium, shifts, receivers):
    plane = medium.shape[1:]
    pad = pltpu.VMEM((4, plane[0] + 2 * TOP, plane[1]), jnp.float32)
    three, four, five, six, seven, eight, ten = [(k, *plane) for k in (3, 4, 5, 6, 7, 8, 10)]
    args = (shifts, background, probes, medium, receivers)
    held = [pltpu.VMEM(v.shape, v.dtype) for v in args[1:]]
    a1 = [None, None]
    a1[0], a1[1], b1, later, inv, waves, row = call(
        start_kernel,
        [five, four, ten, three, four, four, (2, 8, plane[1])],
        [pltpu.SMEM(shifts.shape, shifts.dtype), *held, pad, pltpu.SemaphoreType.DMA((5,))],
        *[pltpu.with_memory_space_constraint(v, pltpu.HBM) for v in args],
        space=pltpu.HBM,
    )
    ra1 = [swap_links(a1[p]) for p in range(2)]
    rb1 = swap_cores(b1)
    a2, ra2, b2 = [None, None], [None, None], []
    for p in range(2):
        a2[p], out_b = call(
            functools.partial(forward_kernel, p),
            [four, eight] if p else [seven, four],
            [pad, pad],
            row, a1[0], a1[p], b1, ra1[0], ra1[p], rb1, inv, b2[0] if p else later,
        )
        b2.append(out_b)
        ra2[p] = swap_links(a2[p])
    rb2 = swap_cores(b2[1])
    a3, ra3, b3 = [None, None], [None, None], []
    right, part_sum = [None, None], [None, None]
    for p in range(2):
        a3[p], out_b, right[p], part_sum[p] = call(
            functools.partial(turn_kernel, p),
            [three, six if p else three, four, four],
            [pad, pad],
            row, a2[p], b2[p], ra2[p], rb2, ra1[0], ra2[0], rb1, later, b1, inv, *b3,
        )
        b3.append(out_b)
        ra3[p] = swap_links(a3[p])
    rb3 = swap_cores(b3[1])
    blocks = lax.axis_size("freq")
    terms = []
    for p in range(2):
        (out,) = call(
            functools.partial(end_kernel, p),
            [(blocks, p + 1, 2, plane[0] // blocks, plane[1])],
            [pad],
            row, a3[p], b3[p], ra3[p], rb3, ra1[0], rb1, inv, right[p], part_sum[p],
            waves, later, b1, *terms,
        )
        terms.append(out)
    return reduced(terms[1])


def solution(mesh):
    in_specs = (
        P(None, "space", None, None),
        P("freq", None, "space", None, None),
        P("space", None, None),
        P("freq", None),
        P("space", None, None),
    )
    out_specs = P(None, "space", "freq", None)
    return jax.shard_map(
        per_device, mesh=mesh, in_specs=in_specs, out_specs=out_specs, check_vma=False
    )
```

```python
import functools

import jax
import jax.numpy as jnp
from jax import lax
from jax.experimental import pallas as pl
from jax.experimental.pallas import tpu as pltpu
from jax.sharding import PartitionSpec as P


OMEGA = 0.8
KEEP = 1.0 - OMEGA
TOP = 8
ROWS = 32


def multiply(x, y):
    return (x[0] * y[0] - x[1] * y[1], x[0] * y[1] + x[1] * y[0])


def multiply_conj(x, y):
    return (x[0] * y[0] + x[1] * y[1], x[0] * y[1] - x[1] * y[0])


def inverse(medium, shift_re, shift_im):
    diag_re = 6.0 + shift_re * medium
    diag_im = shift_im * medium
    scale = OMEGA / (diag_re * diag_re + diag_im * diag_im)
    return (diag_re * scale, -diag_im * scale)


def chunks(height):
    return [(r, min(ROWS, height - r)) for r in range(0, height, ROWS)]


def clear_edges(pad):
    height = pad.shape[-2] - 2 * TOP
    zero = jnp.zeros((TOP, pad.shape[-1]), jnp.float32)
    for part in range(pad.shape[0]):
        pad[part, 0:TOP] = zero
        pad[part, TOP + height :] = zero


def in_plane(pad, part, r, n):
    here = pad[part, TOP + r : TOP + r + n]
    width = here.shape[-1]
    lane = lax.broadcasted_iota(jnp.int32, here.shape, 1)
    left = jnp.where(lane == 0, 0.0, pltpu.roll(here, 1, 1))
    right = jnp.where(lane == width - 1, 0.0, pltpu.roll(here, width - 1, 1))
    above = pad[part, TOP + r - 1 : TOP + r - 1 + n]
    below = pad[part, TOP + r + 1 : TOP + r + 1 + n]
    return here, (left + right) + (above + below)


def complex_in_plane(pad, layer, r, n):
    re, sum_re = in_plane(pad, 2 * layer, r, n)
    im, sum_im = in_plane(pad, 2 * layer + 1, r, n)
    return (re, im), (sum_re, sum_im)


def store(ref, at, r, n, value):
    ref[at, r : r + n] = value[0]
    ref[at + 1, r : r + n] = value[1]


def load(ref, at, r, n):
    return (ref[at, r : r + n], ref[at + 1, r : r + n])


def add(x, y):
    return (x[0] + y[0], x[1] + y[1])


def scale(a, x):
    return (a * x[0], a * x[1])


def side():
    return lax.rem(lax.axis_index("space"), 2)


def has_partner():
    at = lax.axis_index("space")
    last = lax.axis_size("space") - 1
    return jnp.where((at == 0) | (at == last), 0.0, 1.0).astype(jnp.float32)


def first_of(layer, parts, p, r, n):
    if layer == 0:
        return load(parts[p], 0, r, n)
    both = parts[2]
    return scale(both[2 + 4 * p, r : r + n], load(both, 0, r, n))


def partial_of(layer, parts, p, r, n):
    return load(parts[p], 2, r, n) if layer == 0 else load(parts[2], 3 + 4 * p, r, n)


def start_kernel(
    shifts_hbm, back_hbm, probes_hbm, medium_hbm, receivers_hbm,
    out_a0, out_a1, out_b, later, inv, waves, row,
    shifts, back, probes, medium, receivers, pad, sems,
):
    copies = [
        pltpu.make_async_copy(src, dst, sems.at[k])
        for k, (src, dst) in enumerate(
            (
                (shifts_hbm, shifts),
                (medium_hbm, medium),
                (back_hbm, back),
                (probes_hbm, probes),
                (receivers_hbm, receivers),
            )
        )
    ]
    for copy in copies:
        copy.start()
    near = side()
    own = (near, 1 - near)
    height = medium.shape[1]
    medium_at = ((out_a0, 4), (out_b, 5))
    gain_at = ((later, 0), (out_b, 0))
    heard_at = ((later, 2), (out_b, 9))
    clear_edges(pad)
    copies[0].wait()
    shift_re, shift_im = shifts[0, 0], shifts[0, 1]
    row[0] = jnp.full(row.shape[1:], shift_re, jnp.float32)
    row[1] = jnp.full(row.shape[1:], shift_im, jnp.float32)
    copies[1].wait()
    for layer in range(2):
        ref, at = medium_at[layer]
        for r, n in chunks(height):
            med = medium[own[layer], r : r + n]
            store(inv, 2 * layer, r, n, inverse(med, shift_re, shift_im))
            ref[at, r : r + n] = med
    copies[2].wait()
    for layer in range(2):
        ref, at = gain_at[layer]
        for r, n in chunks(height):
            rows = slice(r, r + n)
            bg = (back[0, 0, own[layer], rows], back[0, 1, own[layer], rows])
            wave = multiply((shift_re, shift_im), bg)
            store(waves, 2 * layer, r, n, wave)
            store(ref, at, r, n, multiply(load(inv, 2 * layer, r, n), wave))
    copies[3].wait()
    for p in range(2):
        link = (out_a0, out_a1)[p]
        for layer in range(2):
            gain, at = gain_at[layer]
            for r, n in chunks(height):
                probe = probes[p, own[layer], r : r + n]
                first = scale(probe, load(gain, at, r, n))
                store(pad, 2 * layer, TOP + r, n, first)
                if layer == 0:
                    store(link, 0, r, n, first)
                else:
                    out_b[2 + 4 * p, r : r + n] = probe
        for layer in range(2):
            ref, at = ((link, 2), (out_b, 3 + 4 * p))[layer]
            for r, n in chunks(height):
                here, around = complex_in_plane(pad, layer, r, n)
                around = add(around, load(pad, 2 * (1 - layer), TOP + r, n))
                part = add(scale(1.0 + KEEP, here), multiply(load(inv, 2 * layer, r, n), around))
                store(ref, at, r, n, part)
    copies[4].wait()
    for layer in range(2):
        ref, at = heard_at[layer]
        for r, n in chunks(height):
            ref[at, r : r + n] = receivers[own[layer], r : r + n].astype(jnp.float32)


def halo_inverse(med, layer, row, mask):
    re, im = inverse(med, row[0, 0:1], row[1, 0:1])
    return (mask * re, mask * im) if layer == 0 else (re, im)


def forward_kernel(
    p, row, own_a0, own_a1, own_b, got_a0, got_a1, got_b, inv, extra, *rest
):
    height = inv.shape[1]
    if p == 0:
        out_a, out_b, pad, spare = rest
        out_at = 0
        for k in range(extra.shape[0]):
            for r, n in chunks(height):
                out_a[4 + k, r : r + n] = extra[k, r : r + n]
    else:
        out_a, out_b, pad, spare = rest
        out_at = 4
        out_b[0:4] = extra[...]
    mask = has_partner()
    own = (own_a0, own_a1, own_b)
    got = (got_a0, got_a1, got_b)
    med = ((got_a0, 4), (got_b, 5))
    out = ((out_a, 0), (out_b, out_at))
    clear_edges(pad)
    clear_edges(spare)
    for layer in range(2):
        for r, n in chunks(height):
            second = add(
                partial_of(layer, own, p, r, n),
                multiply(load(inv, 2 * layer, r, n), first_of(layer, got, p, r, n)),
            )
            store(pad, 2 * layer, TOP + r, n, second)
    for layer in range(2):
        for r, n in chunks(height):
            first = first_of(layer, own, p, r, n)
            there = halo_inverse(med[layer][0][med[layer][1], r : r + n], layer, row, mask)
            halo = add(partial_of(layer, got, p, r, n), multiply(there, first))
            here, around = complex_in_plane(pad, layer, r, n)
            around = add(add(around, halo), load(pad, 2 * (1 - layer), TOP + r, n))
            third = add(
                add(scale(KEEP, here), first), multiply(load(inv, 2 * layer, r, n), around)
            )
            store(spare, 2 * layer, TOP + r, n, third)
            store(out[layer][0], out[layer][1], r, n, third)
    for layer in range(2):
        for r, n in chunks(height):
            here, around = complex_in_plane(spare, layer, r, n)
            around = add(around, load(spare, 2 * (1 - layer), TOP + r, n))
            part = add(
                add(scale(KEEP, here), first_of(layer, own, p, r, n)),
                multiply(load(inv, 2 * layer, r, n), around),
            )
            store(out[layer][0], out[layer][1] + 2, r, n, part)


def turn_kernel(
    p, row, own_a, own_b, got_a, got_b, med_a, got_a2, got_b1, later, own_b1, inv, *rest
):
    if p == 0:
        out_a, out_b, right, part_sum, pad, spare = rest
        b_at, out_at = 0, 0
    else:
        first_a, first_b, out_a, out_b, right, part_sum, pad, spare = rest
        b_at, out_at = 4, 3
        out_a[0:3] = first_a[...]
        out_b[0:3] = first_b[...]
    mask = has_partner()
    height = inv.shape[1]
    own = ((own_a, 0), (own_b, 0 if p == 0 else b_at))
    got = ((got_a, 0), (got_b, b_at))
    med = ((med_a, 4), (got_b1, 5))
    rec_own = ((later, 2), (own_b1, 9))
    rec_got = ((got_a2, 6), (got_b1, 9))
    gain = ((got_a2, 4), (got_b1, 0))
    out = ((out_a, out_at), (out_b, out_at))
    clear_edges(pad)
    clear_edges(spare)
    for layer in range(2):
        (mine, at), (theirs, from_) = own[layer], got[layer]
        for r, n in chunks(height):
            there = load(inv, 2 * layer, r, n)
            fourth = add(load(mine, at + 2, r, n), multiply(there, load(theirs, from_, r, n)))
            heard = scale(rec_own[layer][0][rec_own[layer][1], r : r + n], fourth)
            first = multiply_conj(there, heard)
            store(pad, 2 * layer, TOP + r, n, first)
            store(right, 2 * layer, r, n, first)
    for layer in range(2):
        (mine, at), (theirs, from_) = own[layer], got[layer]
        for r, n in chunks(height):
            there = halo_inverse(med[layer][0][med[layer][1], r : r + n], layer, row, mask)
            fourth = add(load(theirs, from_ + 2, r, n), multiply(there, load(mine, at, r, n)))
            halo = multiply_conj(
                there, scale(rec_got[layer][0][rec_got[layer][1], r : r + n], fourth)
            )
            here, around = complex_in_plane(pad, layer, r, n)
            around = add(add(around, halo), load(pad, 2 * (1 - layer), TOP + r, n))
            second = add(
                scale(1.0 + KEEP, here), multiply_conj(load(inv, 2 * layer, r, n), around)
            )
            store(spare, 2 * layer, TOP + r, n, second)
            store(out[layer][0], out[layer][1], r, n, second)
    for layer in range(2):
        for r, n in chunks(height):
            here, around = complex_in_plane(spare, layer, r, n)
            around = add(around, load(spare, 2 * (1 - layer), TOP + r, n))
            part = add(
                add(scale(KEEP, here), load(right, 2 * layer, r, n)),
                multiply_conj(load(inv, 2 * layer, r, n), around),
            )
            store(part_sum, 2 * layer, r, n, part)
            seen = load(*gain[layer], r, n)
            out[layer][0][out[layer][1] + 2, r : r + n] = seen[0] * part[0] + seen[1] * part[1]


def end_kernel(p, row, own_a, own_b, got_a, got_b, med_a, got_b1, inv, right, part_sum, waves, later, own_b1, *rest):
    if p == 0:
        out, pad = rest
        b_at, out_at = 0, 0
    else:
        first_out, out, pad = rest
        b_at, out_at = 3, 1
        out[:, 0:1] = first_out[...]
    mask = has_partner()
    near = side()
    place = (near, 1 - near)
    height = inv.shape[1]
    strip = out.shape[3]
    own = ((own_a, b_at), (own_b, b_at))
    got = ((got_a, b_at), (got_b, b_at))
    med = ((med_a, 4), (got_b1, 5))
    gain = (later, own_b1)
    clear_edges(pad)
    for layer in range(2):
        (mine, at), (theirs, from_) = own[layer], got[layer]
        for r, n in chunks(height):
            third = add(
                load(part_sum, 2 * layer, r, n),
                multiply_conj(load(inv, 2 * layer, r, n), load(theirs, from_, r, n)),
            )
            store(pad, 2 * layer, TOP + r, n, third)
    for layer in range(2):
        (mine, at), (theirs, from_) = own[layer], got[layer]
        for r, n in chunks(height):
            there = halo_inverse(med[layer][0][med[layer][1], r : r + n], layer, row, mask)
            halo = multiply_conj(there, load(mine, at, r, n))
            seen = load(gain[layer], 0, r, n)
            across = theirs[from_ + 2, r : r + n] + (seen[0] * halo[0] + seen[1] * halo[1])
            here, around = complex_in_plane(pad, layer, r, n)
            around = add(around, load(pad, 2 * (1 - layer), TOP + r, n))
            fourth = add(
                add(scale(KEEP, here), load(right, 2 * layer, r, n)),
                multiply_conj(load(inv, 2 * layer, r, n), around),
            )
            wave = load(waves, 2 * layer, r, n)
            term = (wave[0] * fourth[0] + wave[1] * fourth[1]) + across
            for k in range(0, n, strip):
                out[(r + k) // strip, out_at, place[layer]] = term[k : k + strip]


def call(kernel, shapes, scratch, *args, space=pltpu.VMEM):
    vmem = pl.BlockSpec(memory_space=pltpu.VMEM)
    return pl.pallas_call(
        kernel,
        out_shape=[jax.ShapeDtypeStruct(s, jnp.float32) for s in shapes],
        in_specs=[pl.BlockSpec(memory_space=space)] * len(args),
        out_specs=[vmem] * len(shapes),
        scratch_shapes=scratch,
        cost_estimate=pl.CostEstimate(flops=2_000_000, bytes_accessed=2_000_000, transcendentals=0),
        compiler_params=pltpu.CompilerParams(vmem_limit_bytes=16 * 1024 * 1024),
    )(*args)


def swap_links(x):
    count = lax.axis_size("space")
    pairs = []
    for i in range(1, count - 1, 2):
        pairs += [(i, i + 1), (i + 1, i)]
    return lax.ppermute(x, "space", pairs)


def swap_cores(x):
    pairs = []
    for i in range(0, lax.axis_size("space"), 2):
        pairs += [(i, i + 1), (i + 1, i)]
    return lax.ppermute(x, "space", pairs)


def halves_kernel(arrived, keep, send):
    half = lax.rem(lax.axis_index("freq"), 2)
    count = arrived.shape[0] // 2
    for out, at in ((keep, half), (send, 1 - half)):
        for p in range(arrived.shape[1]):
            for layer in range(arrived.shape[2]):
                total = arrived[at, p, layer]
                for k in range(1, count):
                    total = total + arrived[2 * k + at, p, layer]
                out[p, layer] = total


def reduced(terms):
    count = lax.axis_size("freq")
    groups = [list(range(k, count, 2)) for k in range(2)]
    arrived = lax.all_to_all(
        terms, "freq", split_axis=0, concat_axis=0, axis_index_groups=groups, tiled=True
    )
    shape = terms.shape[1:]
    keep, send = call(halves_kernel, [shape, shape], [], arrived)
    pairs = [(k, k ^ 1) for k in range(count)]
    return keep + lax.ppermute(send, "freq", pairs)


def per_device(probes, background, medium, shifts, receivers):
    plane = medium.shape[1:]
    pad = pltpu.VMEM((4, plane[0] + 2 * TOP, plane[1]), jnp.float32)
    three, four, five, six, seven, eight, ten = [(k, *plane) for k in (3, 4, 5, 6, 7, 8, 10)]
    args = (shifts, background, probes, medium, receivers)
    held = [pltpu.VMEM(v.shape, v.dtype) for v in args[1:]]
    a1 = [None, None]
    a1[0], a1[1], b1, later, inv, waves, row = call(
        start_kernel,
        [five, four, ten, three, four, four, (2, 8, plane[1])],
        [pltpu.SMEM(shifts.shape, shifts.dtype), *held, pad, pltpu.SemaphoreType.DMA((5,))],
        *[pltpu.with_memory_space_constraint(v, pltpu.HBM) for v in args],
        space=pltpu.HBM,
    )
    ra1 = [swap_links(a1[p]) for p in range(2)]
    rb1 = swap_cores(b1)
    a2, ra2, b2 = [None, None], [None, None], []
    for p in range(2):
        a2[p], out_b = call(
            functools.partial(forward_kernel, p),
            [four, eight] if p else [seven, four],
            [pad, pad],
            row, a1[0], a1[p], b1, ra1[0], ra1[p], rb1, inv, b2[0] if p else later,
        )
        b2.append(out_b)
        ra2[p] = swap_links(a2[p])
    rb2 = swap_cores(b2[1])
    a3, b3 = [], []
    right, part_sum = [None, None], [None, None]
    for p in range(2):
        out_a, out_b, right[p], part_sum[p] = call(
            functools.partial(turn_kernel, p),
            [six if p else three] * 2 + [four, four],
            [pad, pad],
            row, a2[p], b2[p], ra2[p], rb2, ra1[0], ra2[0], rb1, later, b1, inv, *a3, *b3,
        )
        a3.append(out_a)
        b3.append(out_b)
    ra3 = swap_links(a3[1])
    rb3 = swap_cores(b3[1])
    blocks = lax.axis_size("freq")
    terms = []
    for p in range(2):
        (out,) = call(
            functools.partial(end_kernel, p),
            [(blocks, p + 1, 2, plane[0] // blocks, plane[1])],
            [pad],
            row, a3[p], b3[p], ra3, rb3, ra1[0], rb1, inv, right[p], part_sum[p],
            waves, later, b1, *terms,
        )
        terms.append(out)
    return reduced(terms[1])


def solution(mesh):
    in_specs = (
        P(None, "space", None, None),
        P("freq", None, "space", None, None),
        P("space", None, None),
        P("freq", None),
        P("space", None, None),
    )
    out_specs = P(None, "space", "freq", None)
    return jax.shard_map(
        per_device, mesh=mesh, in_specs=in_specs, out_specs=out_specs, check_vma=False
    )
```
